512 devices in a mesh: groups: 2 (over y), dp: 4 (over x), tensor: 64 (over z, core).
Axes of the slice: x: 4, y: 2, z: 32, core: 2. Of those that a mesh axis runs over, the one named last changes fastest.
The devices are a block of a 4x8x32 slice.
Arguments:
- tokens: bfloat16 [1024, 8192], P(('groups', 'dp'), 'tensor'), parts along dimension 0, may hold values from -6 to 6
- gate_up_weight: bfloat16 [8192, 32768], P('dp', 'tensor'), may hold values from -0.0625 to 0.0625
- down_weight: bfloat16 [16384, 8192], P('tensor', 'dp'), may hold values from -0.046875 to 0.046875
Outputs:
- mixed_out: bfloat16 [1024, 8192], P(('groups', 'dp'), 'tensor'), parts along dimension 0
The draws below stay inside these ranges and needn't reach their ends.
There are 2 independent parts, one for each index of `groups`. The reference program is written for one: setup_inputs(seed, part) draws one part's arguments, and reference() takes and returns one part's arrays. A program takes and returns all parts, laid end to end along the dimension named above; an argument that names none is the same for every part. Nothing has to cross between parts.
All inputs are finite; a program needn't handle non-finite values.
Results may differ from the reference program's by a relative error of at most 0.0049.
Values may be sent and summed in bfloat16 or wider, within the bound.
No kernel may reach another device: no remote copies, remote signals or barrier semaphores. Data moves between devices by JAX's collectives and lax.ppermute only.
A program may use at most 64 MiB of HBM per device.

```python
import jax
import jax.numpy as jnp

D = 8192
FF = 16384
TOKENS = 512


def block_levels(rng, dims, shards, low, top_value):
    def one(axis_at, blocks):
        steps = jax.random.uniform(jax.random.fold_in(jax.random.fold_in(rng, 6), axis_at), (blocks,), jnp.float32, low / len(shards), top_value / len(shards))
        return jnp.repeat(jnp.exp(steps), dims[axis_at] // blocks).reshape((-1,) + (1,) * (len(dims) - axis_at - 1))

    level = one(*shards[0])
    for cut in shards[1:]:
        level = level * one(*cut)
    return level


def bell_draw(stream_key, extent, deviation, bound, shards=(), dtype=jnp.bfloat16):
    entries = deviation * jax.random.normal(stream_key, extent, jnp.float32)
    if shards:
        entries = entries * block_levels(stream_key, extent, shards, -0.22, 0.18)
    return jnp.clip(entries, -bound, bound).astype(dtype)


def setup_inputs(seed: int = 0, part: int = 0) -> dict:
    keys = jax.random.split(jax.random.key(seed), 4)
    part_splits = jax.random.split(jax.random.fold_in(keys[3], part), 4)
    tokens = bell_draw(part_splits[0], (TOKENS, D), 1.0, 6.0, ((0, 4), (1, 64)))
    gate_up_weight = bell_draw(keys[1], (D, 2 * FF), D ** -0.5, 0.0625, ((0, 4), (1, 64)))
    down_weight = bell_draw(keys[2], (FF, D), FF ** -0.5, 0.046875, ((0, 64), (1, 4)))
    return {"tokens": tokens, "gate_up_weight": gate_up_weight, "down_weight": down_weight}


def reference(tokens, gate_up_weight, down_weight):
    combined = jnp.dot(tokens, gate_up_weight, preferred_element_type=jnp.float32)
    gate_part = combined[:, 0::2]
    up_part = combined[:, 1::2]
    hidden = (jax.nn.silu(gate_part) * up_part).astype(jnp.bfloat16)
    return jnp.dot(hidden, down_weight, preferred_element_type=jnp.float32).astype(jnp.bfloat16)
```

```python
import functools

import jax
import jax.numpy as jnp
from jax import lax
from jax.experimental import pallas as pl
from jax.experimental.pallas import tpu as pltpu
from jax.sharding import Mesh
from jax.sharding import PartitionSpec as P

Z = ("zo", "zi")
TENSOR = ("zo", "zi", "core")
F32 = jnp.float32
BF16 = jnp.bfloat16

WINDOW = (-4, -3, -2, -1, 0, 1, 2, 3)


def shifted(array, by):
    n = lax.axis_size(Z)
    return lax.ppermute(array, Z, [(i, (i + by) % n) for i in range(n)])


def swapped(array):
    return lax.ppermute(array, "core", [(0, 1), (1, 0)])


def vmem_call(kernel, outs, *args, flops):
    size = sum(a.size * a.dtype.itemsize for a in (*args, *jax.tree.leaves(outs)))
    return pl.pallas_call(
        kernel,
        out_shape=outs,
        in_specs=[pl.BlockSpec(memory_space=pltpu.VMEM)] * len(args),
        out_specs=jax.tree.map(lambda _: pl.BlockSpec(memory_space=pltpu.VMEM), outs),
        compiler_params=pltpu.CompilerParams(vmem_limit_bytes=40 * 2**20),
        cost_estimate=pl.CostEstimate(flops=flops, bytes_accessed=size, transcendentals=0),
    )(*args)


def up_kernel(mine_refs, theirs_ref, weight_ref, out_ref, rest_ref, total):
    zi, core = lax.axis_index("zi"), lax.axis_index("core")
    n = lax.axis_size("zi")
    width = theirs_ref.shape[2]
    total[...] = jnp.zeros_like(total)
    for i, offset in enumerate(WINDOW):
        residue = lax.rem(zi + (offset + n), n)
        for ref, c in ((mine_refs[i], core), (theirs_ref.at[i], 1 - core)):
            rows = pl.ds(pl.multiple_of((2 * residue + c) * width, width), width)
            total[...] += jnp.dot(ref[...], weight_ref[rows, :], preferred_element_type=F32)
    columns = total.shape[1]
    row = lax.broadcasted_iota(jnp.int32, (columns, columns), 0)
    col = lax.broadcasted_iota(jnp.int32, (columns, columns), 1)
    half = columns // 2
    source = jnp.where(col < half, 2 * col, 2 * (col - half) + 1)
    pick = (row == source).astype(BF16)
    out_ref[...] = jnp.dot(total[...].astype(BF16), pick, preferred_element_type=F32).astype(BF16)
    rows = rest_ref.shape[0]
    stay = total[pl.ds(pl.multiple_of(lax.axis_index("dp") * rows, rows), rows), :]
    rest = (stay - stay.astype(BF16).astype(F32)).astype(BF16)
    rest_ref[...] = jnp.dot(rest, pick, preferred_element_type=F32).astype(BF16)


def hidden_kernel(parts_ref, rest_ref, out_ref):
    total = parts_ref[0].astype(F32) + rest_ref[...].astype(F32)
    for k in range(1, parts_ref.shape[0]):
        total += parts_ref[k].astype(F32)
    half = total.shape[1] // 2
    gate, up = total[:, :half], total[:, half:]
    out_ref[...] = (gate / (1.0 + jnp.exp(-gate)) * up).astype(BF16)


def down_kernel(hidden_ref, other_hidden_ref, weight_ref, other_weight_ref, *out_refs):
    zi, core = lax.axis_index("zi"), lax.axis_index("core")
    n = lax.axis_size("zi")
    width = out_refs[0].shape[1]
    for ref, offset in zip(out_refs, WINDOW):
        residue = lax.rem(zi + (offset + n), n)
        cols = pl.ds(pl.multiple_of((2 * residue + core) * width, width), width)
        term = jnp.dot(hidden_ref[...], weight_ref[:, cols], preferred_element_type=F32)
        term += jnp.dot(other_hidden_ref[...], other_weight_ref[:, cols], preferred_element_type=F32)
        ref[...] = term.astype(ref.dtype)


def per_device(tokens, gate_up_weight, down_weight):
    rows, width = tokens.shape
    dp = lax.axis_size("dp")
    other_weight = swapped(down_weight)
    copies = jnp.broadcast_to(tokens[None], (dp, rows, width))
    copies = lax.all_to_all(copies, "zo", split_axis=0, concat_axis=0, tiled=True)
    block = lax.all_to_all(copies, "dp", split_axis=0, concat_axis=0, tiled=True)
    block = block.reshape(dp * rows, width)
    near = {0: block}
    for s in (2, 1):
        near[-s] = shifted(block, s)
        near[s] = shifted(block, -s)
    near = lax.optimization_barrier(near)
    near[-3] = shifted(near[-2], 1)
    near[-4] = shifted(near[-2], 2)
    near[3] = shifted(near[2], -1)
    mine = [near[o] for o in WINDOW]
    theirs = swapped(jnp.stack(mine))
    columns = gate_up_weight.shape[1]

    def up(*refs):
        up_kernel(refs[: len(WINDOW)], *refs[len(WINDOW) :])

    size = sum(a.size for a in mine) * 4 + gate_up_weight.size * 2
    partial_value, rest = pl.pallas_call(
        up,
        out_shape=(
            jax.ShapeDtypeStruct((dp * rows, columns), BF16),
            jax.ShapeDtypeStruct((rows, columns), BF16),
        ),
        in_specs=[pl.BlockSpec(memory_space=pltpu.VMEM)] * (len(WINDOW) + 2),
        out_specs=(pl.BlockSpec(memory_space=pltpu.VMEM),) * 2,
        scratch_shapes=[pltpu.VMEM((dp * rows, columns), F32)],
        compiler_params=pltpu.CompilerParams(vmem_limit_bytes=40 * 2**20),
        cost_estimate=pl.CostEstimate(
            flops=2 * dp * rows * gate_up_weight.size, bytes_accessed=size, transcendentals=0
        ),
    )(*mine, theirs, gate_up_weight)

    parts = lax.all_to_all(partial_value.reshape(dp, rows, columns), "dp", split_axis=0, concat_axis=0, tiled=True)
    own_hidden = vmem_call(
        hidden_kernel, jax.ShapeDtypeStruct((rows, columns // 2), BF16), parts, rest, flops=10 * parts.size
    )
    hidden = jnp.broadcast_to(own_hidden[None], (dp, *own_hidden.shape))
    hidden = lax.all_to_all(hidden, "dp", split_axis=0, concat_axis=0, tiled=True)
    hidden = hidden.reshape(dp * rows, columns // 2)
    other_hidden = swapped(hidden)

    piece = (dp * rows, width)
    own = vmem_call(
        down_kernel,
        tuple(jax.ShapeDtypeStruct(piece, F32 if o in (-2, 0, 2) else BF16) for o in WINDOW),
        hidden,
        other_hidden,
        down_weight,
        other_weight,
        flops=4 * dp * rows * down_weight.size,
    )
    own = dict(zip(WINDOW, own))
    a2 = shifted(own[-4], -2)
    a1 = shifted(own[-3], -1)
    a3 = shifted(own[3], 1)
    b1 = shifted(own[-1], -1)
    b2 = shifted(own[1], 1)
    b3 = shifted((own[-2] + a1.astype(F32) + a2.astype(F32)).astype(BF16), -2)
    b4 = shifted((own[2] + a3.astype(F32)).astype(BF16), 2)
    window = own[0] + b1.astype(F32) + b2.astype(F32) + b3.astype(F32) + b4.astype(F32)
    out = lax.all_to_all(window.astype(BF16).reshape(dp, rows, width), "dp", split_axis=0, concat_axis=0, tiled=True)
    out = lax.all_to_all(out, "zo", split_axis=0, concat_axis=0, tiled=True)
    return out.astype(F32).sum(axis=0).astype(BF16)


def solution(mesh):
    dp, tensor = mesh.shape["dp"], mesh.shape["tensor"]
    split = Mesh(
        mesh.devices.reshape(mesh.shape["groups"], dp, dp, tensor // (2 * dp), 2),
        ("groups", "dp", *TENSOR),
    )
    placed = (P(("groups", "dp"), TENSOR), P("dp", TENSOR), P(TENSOR, "dp"))
    return jax.shard_map(
        per_device,
        mesh=split,
        in_specs=placed,
        out_specs=P(("groups", "dp"), TENSOR),
        check_vma=False,
    )
```

```python
import jax
import jax.numpy as jnp
from jax import lax
from jax.experimental import pallas as pl
from jax.experimental.pallas import tpu as pltpu
from jax.sharding import Mesh
from jax.sharding import PartitionSpec as P

Z = ("zo", "zi")
TENSOR = ("zo", "zi", "core")
F32 = jnp.float32
BF16 = jnp.bfloat16

STEPS = (1, 2, 3, 4)


def shifted(array, by, cores=(0, 1)):
    n = lax.axis_size(Z)
    pairs = [(2 * i + c, 2 * ((i + (by, -by)[c]) % n) + c) for i in range(n) for c in cores]
    return lax.ppermute(array, TENSOR, pairs)


def residue_at(step, core):
    n = lax.axis_size("zi")
    return lax.rem(lax.axis_index("zi") + jnp.where(core == 0, n - step, step), n)


def whole(start, size):
    return pl.ds(pl.multiple_of(start, size), size)


def swapped(array):
    return lax.ppermute(array, "core", [(0, 1), (1, 0)])


def vmem_call(kernel, outs, *args, flops, scratch=()):
    size = sum(a.size * a.dtype.itemsize for a in (*args, *jax.tree.leaves(outs)))
    return pl.pallas_call(
        kernel,
        out_shape=outs,
        in_specs=[pl.BlockSpec(memory_space=pltpu.VMEM)] * len(args),
        out_specs=jax.tree.map(lambda _: pl.BlockSpec(memory_space=pltpu.VMEM), outs),
        scratch_shapes=scratch,
        compiler_params=pltpu.CompilerParams(vmem_limit_bytes=40 * 2**20),
        cost_estimate=pl.CostEstimate(flops=flops, bytes_accessed=size, transcendentals=0),
    )(*args)


def product(pair_ref, weight_ref, residue):
    pair = jnp.concatenate([pair_ref[0], pair_ref[1]], axis=1)
    width = pair.shape[1]
    return jnp.dot(pair, weight_ref[whole(residue * width, width), :], preferred_element_type=F32)


def near_kernel(own_ref, *refs):
    side_refs, weight_ref, total_ref = refs[:-2], refs[-2], refs[-1]
    core = lax.axis_index("core")
    total_ref[...] = product(own_ref, weight_ref, lax.axis_index("zi"))
    for step, ref in zip(STEPS, side_refs):
        total_ref[...] += product(ref, weight_ref, residue_at(step, core))


def up_kernel(total_in_ref, theirs_ref, weight_ref, out_ref, rest_ref, total):
    core = lax.axis_index("core")
    total[...] = total_in_ref[...]
    for k, step in enumerate(STEPS):
        total[...] += product(theirs_ref.at[k], weight_ref, residue_at(step, 1 - core))
    columns = total.shape[1]
    row = lax.broadcasted_iota(jnp.int32, (columns, columns), 0)
    col = lax.broadcasted_iota(jnp.int32, (columns, columns), 1)
    half = columns // 2
    pick = (row == jnp.where(col < half, 2 * col, 2 * (col - half) + 1)).astype(BF16)
    out_ref[...] = jnp.dot(total[...].astype(BF16), pick, preferred_element_type=F32).astype(BF16)
    rows = rest_ref.shape[0]
    stay = total[whole(lax.axis_index("dp") * rows, rows), :]
    rest = (stay - stay.astype(BF16).astype(F32)).astype(BF16)
    rest_ref[...] = jnp.dot(rest, pick, preferred_element_type=F32).astype(BF16)


def hidden_kernel(parts_ref, rest_ref, out_ref):
    total = parts_ref[0].astype(F32) + rest_ref[...].astype(F32)
    for k in range(1, parts_ref.shape[0]):
        total += parts_ref[k].astype(F32)
    half = total.shape[1] // 2
    gate, up = total[:, :half], total[:, half:]
    out_ref[...] = (gate / (1.0 + jnp.exp(-gate)) * up).astype(BF16)


def down_kernel(hidden_ref, weight_ref, other_weight_ref, four_ref, three_ref, one_ref, two_ref, own_ref):
    core = lax.axis_index("core")
    mine, theirs = hidden_ref.at[core], hidden_ref.at[1 - core]

    def term(start, width):
        cols = pl.ds(pl.multiple_of(start, 128), width)
        out = jnp.dot(mine[...], weight_ref[:, cols], preferred_element_type=F32)
        return out + jnp.dot(theirs[...], other_weight_ref[:, cols], preferred_element_type=F32)

    width = four_ref.shape[1]
    for step, ref in zip(STEPS, (one_ref, two_ref, three_ref, four_ref)):
        ref[...] = term(residue_at(step, core) * width, width).astype(ref.dtype)
    half = own_ref.shape[1]
    own_ref[...] = term(lax.axis_index("zi") * width + core * half, half)


def give_kernel(one_ref, two_ref, out_ref):
    width = out_ref.shape[1]
    cols = whole((1 - lax.axis_index("core")) * width, width)
    out_ref[...] = one_ref[:, cols].astype(F32) + two_ref[:, cols].astype(F32)


def window_kernel(own_ref, one_ref, two_ref, given_ref, out_ref):
    core = lax.axis_index("core")
    width = own_ref.shape[1]
    cols = whole(core * width, width)
    total = own_ref[...] + one_ref[:, cols].astype(F32) + two_ref[:, cols].astype(F32)
    out_ref[...] = (total + given_ref[1 - core]).astype(BF16)


def per_device(tokens, gate_up_weight, down_weight):
    rows, width = tokens.shape
    columns = gate_up_weight.shape[1]
    dp = lax.axis_size("dp")
    shape = jax.ShapeDtypeStruct
    other_weight = swapped(down_weight)
    copies = jnp.broadcast_to(tokens[None], (dp, rows, width))
    copies = lax.all_to_all(copies, "zo", split_axis=0, concat_axis=0, tiled=True)
    block = lax.all_to_all(copies, "dp", split_axis=0, concat_axis=0, tiled=True)
    pair = lax.all_gather(block.reshape(dp * rows, width), "core", axis=0)
    two = shifted(pair, 2)
    one = shifted(pair, 1)
    four = shifted(two, 2, cores=(1,))
    three = shifted(two, 1)
    side = (one, two, three, four)
    theirs = swapped(jnp.stack(side))
    total = vmem_call(
        near_kernel,
        shape((dp * rows, columns), F32),
        pair,
        *side,
        gate_up_weight,
        flops=dp * rows * gate_up_weight.size,
    )
    partial_value, rest = vmem_call(
        up_kernel,
        (shape((dp * rows, columns), BF16), shape((rows, columns), BF16)),
        total,
        theirs,
        gate_up_weight,
        flops=dp * rows * gate_up_weight.size,
        scratch=[pltpu.VMEM((dp * rows, columns), F32)],
    )
    parts = partial_value.reshape(dp, rows, columns)
    parts = lax.all_to_all(parts, "dp", split_axis=0, concat_axis=0, tiled=True)
    own_hidden = vmem_call(
        hidden_kernel, shape((rows, columns // 2), BF16), parts, rest, flops=10 * parts.size
    )
    hidden = jnp.broadcast_to(own_hidden[None], (dp, *own_hidden.shape))
    hidden = lax.all_to_all(hidden, "dp", split_axis=0, concat_axis=0, tiled=True)
    hidden = lax.all_gather(hidden.reshape(dp * rows, columns // 2), "core", axis=0)

    block = (dp * rows, 2 * width)
    four, three, one, two, own = vmem_call(
        down_kernel,
        (shape(block, BF16),) * 3 + (shape(block, F32), shape((dp * rows, width), F32)),
        hidden,
        down_weight,
        other_weight,
        flops=4 * dp * rows * down_weight.size,
    )
    four = shifted(four, -2, cores=(1,))
    three = shifted(three, -1)
    one = shifted(one, -1)
    two = shifted((two + three.astype(F32) + four.astype(F32)).astype(BF16), -2)
    given = vmem_call(give_kernel, shape((dp * rows, width), F32), one, two, flops=2 * own.size)
    given = lax.all_gather(given, "core", axis=0)
    out = vmem_call(window_kernel, shape((dp * rows, width), BF16), own, one, two, given, flops=4 * own.size)
    out = out.reshape(dp, rows, width)
    out = lax.all_to_all(out, "dp", split_axis=0, concat_axis=0, tiled=True)
    out = lax.all_to_all(out, "zo", split_axis=0, concat_axis=0, tiled=True)
    return out.astype(F32).sum(axis=0).astype(BF16)


def solution(mesh):
    dp, tensor = mesh.shape["dp"], mesh.shape["tensor"]
    split = Mesh(
        mesh.devices.reshape(mesh.shape["groups"], dp, dp, tensor // (2 * dp), 2),
        ("groups", "dp", *TENSOR),
    )
    placed = (P(("groups", "dp"), TENSOR), P("dp", TENSOR), P(TENSOR, "dp"))
    return jax.shard_map(
        per_device,
        mesh=split,
        in_specs=placed,
        out_specs=P(("groups", "dp"), TENSOR),
        check_vma=False,
    )
```

```python
import jax
import jax.numpy as jnp
from jax import lax
from jax.experimental import pallas as pl
from jax.experimental.pallas import tpu as pltpu
from jax.sharding import Mesh
from jax.sharding import PartitionSpec as P

Z = ("zo", "zi")
TENSOR = ("zo", "zi", "core")
F32 = jnp.float32
BF16 = jnp.bfloat16

STEPS = (1, 2, 3, 4)


def shifted(array, by, cores=(0, 1)):
    n = lax.axis_size(Z)
    pairs = [(2 * i + c, 2 * ((i + (by, -by)[c]) % n) + c) for i in range(n) for c in cores]
    return lax.ppermute(array, TENSOR, pairs)


def residue_at(step, core):
    n = lax.axis_size("zi")
    return lax.rem(lax.axis_index("zi") + jnp.where(core == 0, n - step, step), n)


def whole(start, size):
    return pl.ds(pl.multiple_of(start, size), size)


def swapped(array):
    return lax.ppermute(array, "core", [(0, 1), (1, 0)])


def vmem_call(kernel, outs, *args, flops, scratch=()):
    size = sum(a.size * a.dtype.itemsize for a in (*args, *jax.tree.leaves(outs)))
    return pl.pallas_call(
        kernel,
        out_shape=outs,
        in_specs=[pl.BlockSpec(memory_space=pltpu.VMEM)] * len(args),
        out_specs=jax.tree.map(lambda _: pl.BlockSpec(memory_space=pltpu.VMEM), outs),
        scratch_shapes=scratch,
        compiler_params=pltpu.CompilerParams(vmem_limit_bytes=40 * 2**20),
        cost_estimate=pl.CostEstimate(flops=flops, bytes_accessed=size, transcendentals=0),
    )(*args)


def product(pair_ref, weight_ref, residue):
    blocks = [jnp.concatenate([pair_ref[k], pair_ref[k + 1]], axis=1) for k in range(0, pair_ref.shape[0], 2)]
    pair = jnp.concatenate(blocks)
    width = pair.shape[1]
    return jnp.dot(pair, weight_ref[whole(residue * width, width), :], preferred_element_type=F32)


def near_kernel(own_ref, *refs):
    side_refs, weight_ref, total_ref = refs[:-2], refs[-2], refs[-1]
    core = lax.axis_index("core")
    total_ref[...] = product(own_ref, weight_ref, lax.axis_index("zi"))
    for step, ref in zip(STEPS, side_refs):
        total_ref[...] += product(ref, weight_ref, residue_at(step, core))


def up_kernel(total_in_ref, theirs_ref, weight_ref, out_ref, rest_ref, total):
    core = lax.axis_index("core")
    total[...] = total_in_ref[...]
    for k, step in enumerate(STEPS):
        total[...] += product(theirs_ref.at[k], weight_ref, residue_at(step, 1 - core))
    columns = total.shape[1]
    row = lax.broadcasted_iota(jnp.int32, (columns, columns), 0)
    col = lax.broadcasted_iota(jnp.int32, (columns, columns), 1)
    half = columns // 2
    pick = (row == jnp.where(col < half, 2 * col, 2 * (col - half) + 1)).astype(BF16)
    out_ref[...] = jnp.dot(total[...].astype(BF16), pick, preferred_element_type=F32).astype(BF16)
    rows = rest_ref.shape[0]
    stay = total[whole(lax.axis_index("dp") * rows, rows), :]
    rest = (stay - stay.astype(BF16).astype(F32)).astype(BF16)
    rest_ref[...] = jnp.dot(rest, pick, preferred_element_type=F32).astype(BF16)


def hidden_kernel(parts_ref, rest_ref, out_ref):
    total = parts_ref[0].astype(F32) + rest_ref[...].astype(F32)
    for k in range(1, parts_ref.shape[0]):
        total += parts_ref[k].astype(F32)
    half = total.shape[1] // 2
    gate, up = total[:, :half], total[:, half:]
    out_ref[...] = (gate / (1.0 + jnp.exp(-gate)) * up).astype(BF16)


def down_kernel(hidden_ref, weight_ref, other_weight_ref, four_ref, three_ref, one_ref, two_ref, own_ref):
    core = lax.axis_index("core")
    mine, theirs = hidden_ref.at[core], hidden_ref.at[1 - core]

    def term(start, width):
        cols = pl.ds(pl.multiple_of(start, 128), width)
        out = jnp.dot(mine[...], weight_ref[:, cols], preferred_element_type=F32)
        return out + jnp.dot(theirs[...], other_weight_ref[:, cols], preferred_element_type=F32)

    width = four_ref.shape[1]
    for step, ref in zip(STEPS, (one_ref, two_ref, three_ref, four_ref)):
        ref[...] = term(residue_at(step, core) * width, width).astype(ref.dtype)
    half = own_ref.shape[1]
    own_ref[...] = term(lax.axis_index("zi") * width + core * half, half)


def give_kernel(one_ref, two_ref, out_ref):
    width = out_ref.shape[1]
    cols = whole((1 - lax.axis_index("core")) * width, width)
    out_ref[...] = one_ref[:, cols].astype(F32) + two_ref[:, cols].astype(F32)


def window_kernel(own_ref, one_ref, two_ref, given_ref, out_ref):
    core = lax.axis_index("core")
    width = own_ref.shape[1]
    cols = whole(core * width, width)
    total = own_ref[...] + one_ref[:, cols].astype(F32) + two_ref[:, cols].astype(F32)
    out_ref[...] = (total + given_ref[1 - core]).astype(BF16)


def per_device(tokens, gate_up_weight, down_weight):
    rows, width = tokens.shape
    columns = gate_up_weight.shape[1]
    dp = lax.axis_size("dp")
    shape = jax.ShapeDtypeStruct
    other_weight = swapped(down_weight)
    copies = lax.all_gather(tokens, "zo", axis=0)
    copies = jnp.repeat(copies, 2, axis=0)
    pair = lax.all_to_all(copies, ("dp", "core"), split_axis=0, concat_axis=0, tiled=True)
    two = shifted(pair, 2)
    one = shifted(pair, 1)
    four = shifted(two, 2, cores=(1,))
    three = shifted(two, 1)
    side = (one, two, three, four)
    theirs = swapped(jnp.stack(side))
    total = vmem_call(
        near_kernel,
        shape((dp * rows, columns), F32),
        pair,
        *side,
        gate_up_weight,
        flops=dp * rows * gate_up_weight.size,
    )
    partial_value, rest = vmem_call(
        up_kernel,
        (shape((dp * rows, columns), BF16), shape((rows, columns), BF16)),
        total,
        theirs,
        gate_up_weight,
        flops=dp * rows * gate_up_weight.size,
        scratch=[pltpu.VMEM((dp * rows, columns), F32)],
    )
    parts = partial_value.reshape(dp, rows, columns)
    parts = lax.all_to_all(parts, "dp", split_axis=0, concat_axis=0, tiled=True)
    own_hidden = vmem_call(
        hidden_kernel, shape((rows, columns // 2), BF16), parts, rest, flops=10 * parts.size
    )
    hidden = jnp.broadcast_to(own_hidden[None], (dp, *own_hidden.shape))
    hidden = lax.all_to_all(hidden, "dp", split_axis=0, concat_axis=0, tiled=True)
    hidden = lax.all_gather(hidden.reshape(dp * rows, columns // 2), "core", axis=0)

    block = (dp * rows, 2 * width)
    four, three, one, two, own = vmem_call(
        down_kernel,
        (shape(block, BF16),) * 3 + (shape(block, F32), shape((dp * rows, width), F32)),
        hidden,
        down_weight,
        other_weight,
        flops=4 * dp * rows * down_weight.size,
    )
    four = shifted(four, -2, cores=(1,))
    three = shifted(three, -1)
    one = shifted(one, -1)
    two = shifted((two + three.astype(F32) + four.astype(F32)).astype(BF16), -2)
    given = vmem_call(give_kernel, shape((dp * rows, width), F32), one, two, flops=2 * own.size)
    given = lax.all_gather(given, "core", axis=0)
    out = vmem_call(window_kernel, shape((dp * rows, width), BF16), own, one, two, given, flops=4 * own.size)
    out = out.reshape(dp, rows, width)
    out = lax.all_to_all(out, "dp", split_axis=0, concat_axis=0, tiled=True)
    out = lax.all_to_all(out, "zo", split_axis=0, concat_axis=0, tiled=True)
    return out.astype(F32).sum(axis=0).astype(BF16)


def solution(mesh):
    dp, tensor = mesh.shape["dp"], mesh.shape["tensor"]
    split = Mesh(
        mesh.devices.reshape(mesh.shape["groups"], dp, dp, tensor // (2 * dp), 2),
        ("groups", "dp", *TENSOR),
    )
    placed = (P(("groups", "dp"), TENSOR), P("dp", TENSOR), P(TENSOR, "dp"))
    return jax.shard_map(
        per_device,
        mesh=split,
        in_specs=placed,
        out_specs=P(("groups", "dp"), TENSOR),
        check_vma=False,
    )
```

```python
import jax
import jax.numpy as jnp
from jax import lax
from jax.experimental import pallas as pl
from jax.experimental.pallas import tpu as pltpu
from jax.sharding import Mesh
from jax.sharding import PartitionSpec as P

Z = ("zo", "zi")
TENSOR = ("zo", "zi", "core")
F32 = jnp.float32
BF16 = jnp.bfloat16

STEPS = (1, 2, 3, 4)


def shifted(array, by, cores=(0, 1)):
    n = lax.axis_size(Z)
    pairs = [(2 * i + c, 2 * ((i + (by, -by)[c]) % n) + c) for i in range(n) for c in cores]
    return lax.ppermute(array, TENSOR, pairs)


def residue_at(step, core):
    n = lax.axis_size("zi")
    return lax.rem(lax.axis_index("zi") + jnp.where(core == 0, n - step, step), n)


def whole(start, size):
    return pl.ds(pl.multiple_of(start, size), size)


def swapped(array):
    return lax.ppermute(array, "core", [(0, 1), (1, 0)])


def vmem_call(kernel, outs, *args, flops, scratch=()):
    size = sum(a.size * a.dtype.itemsize for a in (*args, *jax.tree.leaves(outs)))
    return pl.pallas_call(
        kernel,
        out_shape=outs,
        in_specs=[pl.BlockSpec(memory_space=pltpu.VMEM)] * len(args),
        out_specs=jax.tree.map(lambda _: pl.BlockSpec(memory_space=pltpu.VMEM), outs),
        scratch_shapes=scratch,
        compiler_params=pltpu.CompilerParams(vmem_limit_bytes=40 * 2**20),
        cost_estimate=pl.CostEstimate(flops=flops, bytes_accessed=size, transcendentals=0),
    )(*args)


def product(pair_ref, weight_ref, residue):
    blocks = [jnp.concatenate([pair_ref[k], pair_ref[k + 1]], axis=1) for k in range(0, pair_ref.shape[0], 2)]
    pair = jnp.concatenate(blocks)
    width = pair.shape[1]
    return jnp.dot(pair, weight_ref[whole(residue * width, width), :], preferred_element_type=F32)


def near_kernel(own_ref, *refs):
    side_refs, weight_ref, total_ref = refs[:-2], refs[-2], refs[-1]
    core = lax.axis_index("core")
    total_ref[...] = product(own_ref, weight_ref, lax.axis_index("zi"))
    for step, ref in zip(STEPS, side_refs):
        total_ref[...] += product(ref, weight_ref, residue_at(step, core))


def up_kernel(total_in_ref, theirs_ref, weight_ref, out_ref, rest_ref, total):
    core = lax.axis_index("core")
    total[...] = total_in_ref[...]
    for k, step in enumerate(STEPS):
        total[...] += product(theirs_ref.at[k], weight_ref, residue_at(step, 1 - core))
    columns = total.shape[1]
    row = lax.broadcasted_iota(jnp.int32, (columns, columns), 0)
    col = lax.broadcasted_iota(jnp.int32, (columns, columns), 1)
    half = columns // 2
    pick = (row == jnp.where(col < half, 2 * col, 2 * (col - half) + 1)).astype(BF16)
    out_ref[...] = jnp.dot(total[...].astype(BF16), pick, preferred_element_type=F32).astype(BF16)
    rows = rest_ref.shape[0]
    stay = total[whole(lax.axis_index("dp") * rows, rows), :]
    rest = (stay - stay.astype(BF16).astype(F32)).astype(BF16)
    rest_ref[...] = jnp.dot(rest, pick, preferred_element_type=F32).astype(BF16)


def hidden_kernel(parts_ref, rest_ref, out_ref):
    total = parts_ref[0].astype(F32) + rest_ref[...].astype(F32)
    for k in range(1, parts_ref.shape[0]):
        total += parts_ref[k].astype(F32)
    half = total.shape[1] // 2
    gate, up = total[:, :half], total[:, half:]
    out_ref[...] = (gate / (1.0 + jnp.exp(-gate)) * up).astype(BF16)


def down_kernel(hidden_ref, weight_ref, other_weight_ref, four_ref, three_ref, one_ref, two_ref, own_ref):
    core = lax.axis_index("core")
    mine, theirs = hidden_ref.at[core], hidden_ref.at[1 - core]

    def term(start, width):
        cols = pl.ds(pl.multiple_of(start, 128), width)
        out = jnp.dot(mine[...], weight_ref[:, cols], preferred_element_type=F32)
        return out + jnp.dot(theirs[...], other_weight_ref[:, cols], preferred_element_type=F32)

    width = four_ref.shape[1]
    for step, ref in zip(STEPS, (one_ref, two_ref, three_ref, four_ref)):
        ref[...] = term(residue_at(step, core) * width, width).astype(ref.dtype)
    half = own_ref.shape[1]
    own_ref[...] = term(lax.axis_index("zi") * width + core * half, half)


def give_kernel(one_ref, two_ref, out_ref):
    width = out_ref.shape[1]
    cols = whole((1 - lax.axis_index("core")) * width, width)
    out_ref[...] = one_ref[:, cols].astype(F32) + two_ref[:, cols].astype(F32)


def window_kernel(own_ref, one_ref, two_ref, given_ref, out_ref):
    core = lax.axis_index("core")
    width = own_ref.shape[1]
    cols = whole(core * width, width)
    total = own_ref[...] + one_ref[:, cols].astype(F32) + two_ref[:, cols].astype(F32)
    out_ref[...] = (total + given_ref[1 - core]).astype(BF16)


def per_device(tokens, gate_up_weight, down_weight):
    rows, width = tokens.shape
    columns = gate_up_weight.shape[1]
    dp = lax.axis_size("dp")
    shape = jax.ShapeDtypeStruct
    other_weight = swapped(down_weight)
    copies = jnp.broadcast_to(tokens[None], (dp, rows, width))
    copies = lax.all_to_all(copies, "zo", split_axis=0, concat_axis=0, tiled=True)
    copies = jnp.repeat(copies, 2, axis=0)
    pair = lax.all_to_all(copies, ("dp", "core"), split_axis=0, concat_axis=0, tiled=True)
    two = shifted(pair, 2)
    one = shifted(pair, 1)
    two, other_weight = lax.optimization_barrier((two, other_weight))
    four = shifted(two, 2, cores=(1,))
    three = shifted(two, 1)
    side = (one, two, three, four)
    theirs = swapped(jnp.stack(side))
    total = vmem_call(
        near_kernel,
        shape((dp * rows, columns), F32),
        pair,
        *side,
        gate_up_weight,
        flops=dp * rows * gate_up_weight.size,
    )
    partial_value, rest = vmem_call(
        up_kernel,
        (shape((dp * rows, columns), BF16), shape((rows, columns), BF16)),
        total,
        theirs,
        gate_up_weight,
        flops=dp * rows * gate_up_weight.size,
        scratch=[pltpu.VMEM((dp * rows, columns), F32)],
    )
    parts = partial_value.reshape(dp, rows, columns)
    parts = lax.all_to_all(parts, "dp", split_axis=0, concat_axis=0, tiled=True)
    own_hidden = vmem_call(
        hidden_kernel, shape((rows, columns // 2), BF16), parts, rest, flops=10 * parts.size
    )
    hidden = jnp.broadcast_to(own_hidden[None], (dp, *own_hidden.shape))
    hidden = lax.all_to_all(hidden, "dp", split_axis=0, concat_axis=0, tiled=True)
    hidden = lax.all_gather(hidden.reshape(dp * rows, columns // 2), "core", axis=0)

    block = (dp * rows, 2 * width)
    four, three, one, two, own = vmem_call(
        down_kernel,
        (shape(block, BF16),) * 3 + (shape(block, F32), shape((dp * rows, width), F32)),
        hidden,
        down_weight,
        other_weight,
        flops=4 * dp * rows * down_weight.size,
    )
    four = shifted(four, -2, cores=(1,))
    three = shifted(three, -1)
    one = shifted(one, -1)
    two = shifted((two + three.astype(F32) + four.astype(F32)).astype(BF16), -2)
    given = vmem_call(give_kernel, shape((dp * rows, width), F32), one, two, flops=2 * own.size)
    given = lax.all_gather(given, "core", axis=0)
    out = vmem_call(window_kernel, shape((dp * rows, width), BF16), own, one, two, given, flops=4 * own.size)
    out = out.reshape(dp, rows, width)
    out = lax.all_to_all(out, "dp", split_axis=0, concat_axis=0, tiled=True)
    out = lax.all_to_all(out, "zo", split_axis=0, concat_axis=0, tiled=True)
    return out.astype(F32).sum(axis=0).astype(BF16)


def solution(mesh):
    dp, tensor = mesh.shape["dp"], mesh.shape["tensor"]
    split = Mesh(
        mesh.devices.reshape(mesh.shape["groups"], dp, dp, tensor // (2 * dp), 2),
        ("groups", "dp", *TENSOR),
    )
    placed = (P(("groups", "dp"), TENSOR), P("dp", TENSOR), P(TENSOR, "dp"))
    return jax.shard_map(
        per_device,
        mesh=split,
        in_specs=placed,
        out_specs=P(("groups", "dp"), TENSOR),
        check_vma=False,
    )
```

```python
import jax
import jax.numpy as jnp
from jax import lax
from jax.experimental import pallas as pl
from jax.experimental.pallas import tpu as pltpu
from jax.sharding import Mesh
from jax.sharding import PartitionSpec as P


Z = ("zo", "zi")
TENSOR = ("zo", "zi", "core")
F32 = jnp.float32
BF16 = jnp.bfloat16

STEPS = (1, 2, 3, 4)


def shifted(array, by, cores=(0, 1)):
    n = lax.axis_size(Z)
    pairs = [(2 * i + c, 2 * ((i + (by, -by)[c]) % n) + c) for i in range(n) for c in cores]
    return lax.ppermute(array, TENSOR, pairs)


def residue_at(step, core):
    n = lax.axis_size("zi")
    return lax.rem(lax.axis_index("zi") + jnp.where(core == 0, n - step, step), n)


def whole(start, size):
    return pl.ds(pl.multiple_of(start, size), size)


def swapped(array):
    return lax.ppermute(array, "core", [(0, 1), (1, 0)])


def vmem_call(kernel, outs, *args, flops, scratch=()):
    vmem = pl.BlockSpec(memory_space=pltpu.VMEM)
    flat, tree = jax.tree.flatten(args)
    size = sum(a.size * a.dtype.itemsize for a in (*flat, *jax.tree.leaves(outs)))

    def body(*refs):
        kernel(*jax.tree.unflatten(tree, refs[: len(flat)]), *refs[len(flat) :])

    return pl.pallas_call(
        body,
        out_shape=outs,
        in_specs=[vmem] * len(flat),
        out_specs=jax.tree.map(lambda _: vmem, outs),
        scratch_shapes=scratch,
        compiler_params=pltpu.CompilerParams(vmem_limit_bytes=40 * 2**20),
        cost_estimate=pl.CostEstimate(flops=flops, bytes_accessed=size, transcendentals=0),
    )(*flat)


def add_product(total, ref, at, half, weight_ref, residue):
    blocks = range(at, at + lax.axis_size("dp"), 2)
    data = jnp.concatenate([jnp.concatenate([ref[k], ref[k + 1]], axis=1) for k in blocks])
    rows, width = data.shape
    weight = weight_ref[whole(residue * width, width), :]
    total[whole(half * rows, rows), :] += jnp.dot(data, weight, preferred_element_type=F32)


def near_kernel(own_ref, one_ref, two_refs, three_refs, four_ref, weight_ref, total):
    core, n = lax.axis_index("core"), lax.axis_size("dp")
    total[...] = jnp.zeros_like(total)
    for half in (0, 1):
        add_product(total, own_ref, half * n, half, weight_ref, lax.axis_index("zi"))
        add_product(total, one_ref, half * n, half, weight_ref, residue_at(1, core))
    for step, refs in ((2, two_refs), (3, three_refs), (4, (four_ref,))):
        for ref, half in zip(refs, (core, 1 - core)):
            add_product(total, ref, 0, half, weight_ref, residue_at(step, core))


def up_kernel(total_in_ref, theirs_ref, weight_ref, out_ref, rest_ref, total):
    core, n = lax.axis_index("core"), lax.axis_size("dp")
    total[...] = total_in_ref[...]
    halves = (1, 0), (1, 1), (2, 1 - core), (2, core), (3, 1 - core), (3, core), (4, 1 - core)
    for k, (step, half) in enumerate(halves):
        add_product(total, theirs_ref, k * n, half, weight_ref, residue_at(step, 1 - core))
    columns = total.shape[1]
    row = lax.broadcasted_iota(jnp.int32, (columns, columns), 0)
    col = lax.broadcasted_iota(jnp.int32, (columns, columns), 1)
    half = columns // 2
    pick = (row == jnp.where(col < half, 2 * col, 2 * (col - half) + 1)).astype(BF16)
    out_ref[...] = jnp.dot(total[...].astype(BF16), pick, preferred_element_type=F32).astype(BF16)
    rows = rest_ref.shape[0]
    stay = total[whole(lax.axis_index("dp") * rows, rows), :]
    rest = (stay - stay.astype(BF16).astype(F32)).astype(BF16)
    rest_ref[...] = jnp.dot(rest, pick, preferred_element_type=F32).astype(BF16)


def hidden_kernel(parts_ref, rest_ref, out_ref):
    total = parts_ref[0].astype(F32) + rest_ref[...].astype(F32)
    for k in range(1, parts_ref.shape[0]):
        total += parts_ref[k].astype(F32)
    half = total.shape[1] // 2
    gate, up = total[:, :half], total[:, half:]
    out_ref[...] = (gate / (1.0 + jnp.exp(-gate)) * up).astype(BF16)


def down_kernel(hidden_ref, weight_ref, other_weight_ref, four_ref, three_ref, one_ref, two_ref, own_ref):
    core = lax.axis_index("core")
    mine, theirs = hidden_ref.at[core], hidden_ref.at[1 - core]

    def term(start, width):
        cols = pl.ds(pl.multiple_of(start, 128), width)
        out = jnp.dot(mine[...], weight_ref[:, cols], preferred_element_type=F32)
        return out + jnp.dot(theirs[...], other_weight_ref[:, cols], preferred_element_type=F32)

    width = four_ref.shape[1]
    for step, ref in zip(STEPS, (one_ref, two_ref, three_ref, four_ref)):
        ref[...] = term(residue_at(step, core) * width, width).astype(ref.dtype)
    half = own_ref.shape[1]
    own_ref[...] = term(lax.axis_index("zi") * width + core * half, half)


def give_kernel(one_ref, two_ref, out_ref):
    width = out_ref.shape[1]
    cols = whole((1 - lax.axis_index("core")) * width, width)
    out_ref[...] = one_ref[:, cols].astype(F32) + two_ref[:, cols].astype(F32)


def window_kernel(own_ref, one_ref, two_ref, given_ref, out_ref):
    core = lax.axis_index("core")
    width = own_ref.shape[1]
    cols = whole(core * width, width)
    total = own_ref[...] + one_ref[:, cols].astype(F32) + two_ref[:, cols].astype(F32)
    out_ref[...] = (total + given_ref[1 - core]).astype(BF16)


def per_device(tokens, gate_up_weight, down_weight):
    rows, width = tokens.shape
    columns = gate_up_weight.shape[1]
    dp = lax.axis_size("dp")
    shape = jax.ShapeDtypeStruct
    other_weight = swapped(down_weight)
    copies = jnp.broadcast_to(tokens[None], (dp, rows, width))
    copies = lax.all_to_all(copies, "zo", split_axis=0, concat_axis=0, tiled=True)
    copies = jnp.repeat(copies, 2, axis=0)
    pair = lax.all_to_all(copies, ("dp", "core"), split_axis=0, concat_axis=0, tiled=True)
    core = lax.axis_index("core")
    halves = pair.reshape(2, dp, rows, width)
    first = jnp.where(core == 0, halves[0], halves[1])
    second = jnp.where(core == 0, halves[1], halves[0])
    first, second, pair = lax.optimization_barrier((first, second, pair))
    first = shifted(first, 2)
    second = shifted(second, 2)
    one = shifted(pair, 1)
    first, other_weight = lax.optimization_barrier((first, other_weight))
    four = shifted(first, 2)
    two = (first, second)
    three = (shifted(first, 1), shifted(second, 1))
    theirs = swapped(jnp.concatenate([one, *two, *three, four]))
    total = vmem_call(
        near_kernel,
        shape((dp * rows, columns), F32),
        pair,
        one,
        two,
        three,
        four,
        gate_up_weight,
        flops=dp * rows * gate_up_weight.size,
    )
    partial_value, rest = vmem_call(
        up_kernel,
        (shape((dp * rows, columns), BF16), shape((rows, columns), BF16)),
        total,
        theirs,
        gate_up_weight,
        flops=dp * rows * gate_up_weight.size,
        scratch=[pltpu.VMEM((dp * rows, columns), F32)],
    )
    parts = partial_value.reshape(dp, rows, columns)
    parts = lax.all_to_all(parts, "dp", split_axis=0, concat_axis=0, tiled=True)
    own_hidden = vmem_call(
        hidden_kernel, shape((rows, columns // 2), BF16), parts, rest, flops=10 * parts.size
    )
    hidden = jnp.broadcast_to(own_hidden[None], (dp, *own_hidden.shape))
    hidden = lax.all_to_all(hidden, "dp", split_axis=0, concat_axis=0, tiled=True)
    hidden = lax.all_gather(hidden.reshape(dp * rows, columns // 2), "core", axis=0)

    block = (dp * rows, 2 * width)
    four, three, one, two, own = vmem_call(
        down_kernel,
        (shape(block, BF16),) * 3 + (shape(block, F32), shape((dp * rows, width), F32)),
        hidden,
        down_weight,
        other_weight,
        flops=4 * dp * rows * down_weight.size,
    )
    four = shifted(four, -2, cores=(1,))
    three = shifted(three, -1)
    one = shifted(one, -1)
    two = shifted((two + three.astype(F32) + four.astype(F32)).astype(BF16), -2)
    given = vmem_call(give_kernel, shape((dp * rows, width), F32), one, two, flops=2 * own.size)
    given = lax.all_gather(given, "core", axis=0)
    out = vmem_call(window_kernel, shape((dp * rows, width), BF16), own, one, two, given, flops=4 * own.size)
    out = out.reshape(dp, rows, width)
    out = lax.all_to_all(out, "dp", split_axis=0, concat_axis=0, tiled=True)
    out = lax.all_to_all(out, "zo", split_axis=0, concat_axis=0, tiled=True)
    return out.astype(F32).sum(axis=0).astype(BF16)


def solution(mesh):
    dp, tensor = mesh.shape["dp"], mesh.shape["tensor"]
    split = Mesh(
        mesh.devices.reshape(mesh.shape["groups"], dp, dp, tensor // (2 * dp), 2),
        ("groups", "dp", *TENSOR),
    )
    placed = (P(("groups", "dp"), TENSOR), P("dp", TENSOR), P(TENSOR, "dp"))
    return jax.shard_map(
        per_device,
        mesh=split,
        in_specs=placed,
        out_specs=P(("groups", "dp"), TENSOR),
        check_vma=False,
    )
```

```python
import jax
import jax.numpy as jnp
from jax import lax
from jax.experimental import pallas as pl
from jax.experimental.pallas import tpu as pltpu
from jax.sharding import Mesh
from jax.sharding import PartitionSpec as P


Z = ("zo", "zi")
TENSOR = ("zo", "zi", "core")
F32 = jnp.float32
BF16 = jnp.bfloat16

STEPS = (1, 2, 3, 4)


def shifted(array, by, cores=(0, 1)):
    n = lax.axis_size(Z)
    pairs = [(2 * i + c, 2 * ((i + (by, -by)[c]) % n) + c) for i in range(n) for c in cores]
    return lax.ppermute(array, TENSOR, pairs)


def residue_at(step, core):
    n = lax.axis_size("zi")
    return lax.rem(lax.axis_index("zi") + jnp.where(core == 0, n - step, step), n)


def whole(start, size):
    return pl.ds(pl.multiple_of(start, size), size)


def swapped(array):
    return lax.ppermute(array, "core", [(0, 1), (1, 0)])


def vmem_call(kernel, outs, *args, flops, scratch=()):
    vmem = pl.BlockSpec(memory_space=pltpu.VMEM)
    flat, tree = jax.tree.flatten(args)
    size = sum(a.size * a.dtype.itemsize for a in (*flat, *jax.tree.leaves(outs)))

    def body(*refs):
        kernel(*jax.tree.unflatten(tree, refs[: len(flat)]), *refs[len(flat) :])

    return pl.pallas_call(
        body,
        out_shape=outs,
        in_specs=[vmem] * len(flat),
        out_specs=jax.tree.map(lambda _: vmem, outs),
        scratch_shapes=scratch,
        compiler_params=pltpu.CompilerParams(vmem_limit_bytes=40 * 2**20),
        cost_estimate=pl.CostEstimate(flops=flops, bytes_accessed=size, transcendentals=0),
    )(*flat)


def add_product(total, ref, at, half, weight_ref, residue):
    blocks = range(at, at + lax.axis_size("dp"), 2)
    data = jnp.concatenate([jnp.concatenate([ref[k], ref[k + 1]], axis=1) for k in blocks])
    rows, width = data.shape
    weight = weight_ref[whole(residue * width, width), :]
    total[whole(half * rows, rows), :] += jnp.dot(data, weight, preferred_element_type=F32)


def near_kernel(own_ref, one_ref, two_refs, three_ref, four_refs, weight_ref, total):
    core, n = lax.axis_index("core"), lax.axis_size("dp")
    total[...] = jnp.zeros_like(total)
    for half in (0, 1):
        add_product(total, own_ref, half * n, half, weight_ref, lax.axis_index("zi"))
        add_product(total, one_ref, half * n, half, weight_ref, residue_at(1, core))
        add_product(total, two_refs[half], 0, half, weight_ref, residue_at(2, core))
        add_product(total, three_ref, half * n, half, weight_ref, residue_at(3, core))
        add_product(total, four_refs[half], 0, half, weight_ref, residue_at(4, core))


def up_kernel(total_in_ref, theirs_ref, weight_ref, out_ref, rest_ref, total):
    core, n = lax.axis_index("core"), lax.axis_size("dp")
    total[...] = total_in_ref[...]
    for k in range(8):
        add_product(total, theirs_ref, k * n, k % 2, weight_ref, residue_at(k // 2 + 1, 1 - core))
    columns = total.shape[1]
    row = lax.broadcasted_iota(jnp.int32, (columns, columns), 0)
    col = lax.broadcasted_iota(jnp.int32, (columns, columns), 1)
    half = columns // 2
    pick = (row == jnp.where(col < half, 2 * col, 2 * (col - half) + 1)).astype(BF16)
    out_ref[...] = jnp.dot(total[...].astype(BF16), pick, preferred_element_type=F32).astype(BF16)
    rows = rest_ref.shape[0]
    stay = total[whole(lax.axis_index("dp") * rows, rows), :]
    rest = (stay - stay.astype(BF16).astype(F32)).astype(BF16)
    rest_ref[...] = jnp.dot(rest, pick, preferred_element_type=F32).astype(BF16)


def hidden_kernel(parts_ref, rest_ref, out_ref):
    total = parts_ref[0].astype(F32) + rest_ref[...].astype(F32)
    for k in range(1, parts_ref.shape[0]):
        total += parts_ref[k].astype(F32)
    half = total.shape[1] // 2
    gate, up = total[:, :half], total[:, half:]
    out_ref[...] = (gate / (1.0 + jnp.exp(-gate)) * up).astype(BF16)


def down_kernel(hidden_ref, weight_ref, other_weight_ref, four_ref, three_ref, one_ref, two_ref, own_ref):
    core = lax.axis_index("core")
    mine, theirs = hidden_ref.at[core], hidden_ref.at[1 - core]

    def term(start, width):
        cols = pl.ds(pl.multiple_of(start, 128), width)
        out = jnp.dot(mine[...], weight_ref[:, cols], preferred_element_type=F32)
        return out + jnp.dot(theirs[...], other_weight_ref[:, cols], preferred_element_type=F32)

    width = four_ref.shape[1]
    for step, ref in zip(STEPS, (one_ref, two_ref, three_ref, four_ref)):
        ref[...] = term(residue_at(step, core) * width, width).astype(ref.dtype)
    half = own_ref.shape[1]
    own_ref[...] = term(lax.axis_index("zi") * width + core * half, half)


def give_kernel(one_ref, two_ref, out_ref):
    width = out_ref.shape[1]
    cols = whole((1 - lax.axis_index("core")) * width, width)
    out_ref[...] = one_ref[:, cols].astype(F32) + two_ref[:, cols].astype(F32)


def window_kernel(own_ref, one_ref, two_ref, given_ref, out_ref):
    core = lax.axis_index("core")
    width = own_ref.shape[1]
    cols = whole(core * width, width)
    total = own_ref[...] + one_ref[:, cols].astype(F32) + two_ref[:, cols].astype(F32)
    out_ref[...] = (total + given_ref[1 - core]).astype(BF16)


def per_device(tokens, gate_up_weight, down_weight):
    rows, width = tokens.shape
    columns = gate_up_weight.shape[1]
    dp = lax.axis_size("dp")
    shape = jax.ShapeDtypeStruct
    other_weight = swapped(down_weight)
    copies = lax.all_gather(tokens, "zo", axis=0)
    copies = jnp.repeat(copies, 2, axis=0)
    pair = lax.all_to_all(copies, ("dp", "core"), split_axis=0, concat_axis=0, tiled=True)
    halves = (pair[:dp], pair[dp:])
    halves, pair = lax.optimization_barrier((halves, pair))
    first = shifted(halves[0], 2)
    second = shifted(halves[1], 2)
    one = shifted(pair, 1)
    first, other_weight = lax.optimization_barrier((first, other_weight))
    two = (first, second)
    four = tuple(shifted(a, 2, cores=(1,)) for a in two)
    three = shifted(jnp.concatenate(two), 1)
    theirs = swapped(jnp.concatenate([one, *two, three, *four]))
    total = vmem_call(
        near_kernel,
        shape((dp * rows, columns), F32),
        pair,
        one,
        two,
        three,
        four,
        gate_up_weight,
        flops=dp * rows * gate_up_weight.size,
    )
    partial_value, rest = vmem_call(
        up_kernel,
        (shape((dp * rows, columns), BF16), shape((rows, columns), BF16)),
        total,
        theirs,
        gate_up_weight,
        flops=dp * rows * gate_up_weight.size,
        scratch=[pltpu.VMEM((dp * rows, columns), F32)],
    )
    parts = partial_value.reshape(dp, rows, columns)
    parts = lax.all_to_all(parts, "dp", split_axis=0, concat_axis=0, tiled=True)
    own_hidden = vmem_call(
        hidden_kernel, shape((rows, columns // 2), BF16), parts, rest, flops=10 * parts.size
    )
    hidden = jnp.broadcast_to(own_hidden[None], (dp, *own_hidden.shape))
    hidden = lax.all_to_all(hidden, "dp", split_axis=0, concat_axis=0, tiled=True)
    hidden = lax.all_gather(hidden.reshape(dp * rows, columns // 2), "core", axis=0)

    block = (dp * rows, 2 * width)
    four, three, one, two, own = vmem_call(
        down_kernel,
        (shape(block, BF16),) * 3 + (shape(block, F32), shape((dp * rows, width), F32)),
        hidden,
        down_weight,
        other_weight,
        flops=4 * dp * rows * down_weight.size,
    )
    four = shifted(four, -2, cores=(1,))
    three = shifted(three, -1)
    one = shifted(one, -1)
    two = shifted((two + three.astype(F32) + four.astype(F32)).astype(BF16), -2)
    given = vmem_call(give_kernel, shape((dp * rows, width), F32), one, two, flops=2 * own.size)
    given = lax.all_gather(given, "core", axis=0)
    out = vmem_call(window_kernel, shape((dp * rows, width), BF16), own, one, two, given, flops=4 * own.size)
    out = out.reshape(dp, rows, width)
    out = lax.all_to_all(out, "dp", split_axis=0, concat_axis=0, tiled=True)
    out = lax.all_to_all(out, "zo", split_axis=0, concat_axis=0, tiled=True)
    return out.astype(F32).sum(axis=0).astype(BF16)


def solution(mesh):
    dp, tensor = mesh.shape["dp"], mesh.shape["tensor"]
    split = Mesh(
        mesh.devices.reshape(mesh.shape["groups"], dp, dp, tensor // (2 * dp), 2),
        ("groups", "dp", *TENSOR),
    )
    placed = (P(("groups", "dp"), TENSOR), P("dp", TENSOR), P(TENSOR, "dp"))
    return jax.shard_map(
        per_device,
        mesh=split,
        in_specs=placed,
        out_specs=P(("groups", "dp"), TENSOR),
        check_vma=False,
    )
```

```python
import jax
import jax.numpy as jnp
from jax import lax
from jax.experimental import pallas as pl
from jax.experimental.pallas import tpu as pltpu
from jax.sharding import Mesh
from jax.sharding import PartitionSpec as P


Z = ("zo", "zi")
TENSOR = ("zo", "zi", "core")
F32 = jnp.float32
BF16 = jnp.bfloat16

STEPS = (1, 2, 3, 4)


def shifted(array, by, cores=(0, 1)):
    n = lax.axis_size(Z)
    pairs = [(2 * i + c, 2 * ((i + (by, -by)[c]) % n) + c) for i in range(n) for c in cores]
    return lax.ppermute(array, TENSOR, pairs)


def residue_at(step, core):
    n = lax.axis_size("zi")
    return lax.rem(lax.axis_index("zi") + jnp.where(core == 0, n - step, step), n)


def whole(start, size):
    return pl.ds(pl.multiple_of(start, size), size)


def swapped(array):
    return lax.ppermute(array, "core", [(0, 1), (1, 0)])


def vmem_call(kernel, outs, *args, flops, scratch=()):
    vmem = pl.BlockSpec(memory_space=pltpu.VMEM)
    flat, tree = jax.tree.flatten(args)
    size = sum(a.size * a.dtype.itemsize for a in (*flat, *jax.tree.leaves(outs)))

    def body(*refs):
        kernel(*jax.tree.unflatten(tree, refs[: len(flat)]), *refs[len(flat) :])

    return pl.pallas_call(
        body,
        out_shape=outs,
        in_specs=[vmem] * len(flat),
        out_specs=jax.tree.map(lambda _: vmem, outs),
        scratch_shapes=scratch,
        compiler_params=pltpu.CompilerParams(vmem_limit_bytes=40 * 2**20),
        cost_estimate=pl.CostEstimate(flops=flops, bytes_accessed=size, transcendentals=0),
    )(*flat)


def add_product(total, ref, at, half, weight_ref, residue):
    blocks = range(at, at + lax.axis_size("dp"), 2)
    data = jnp.concatenate([jnp.concatenate([ref[k], ref[k + 1]], axis=1) for k in blocks])
    rows, width = data.shape
    weight = weight_ref[whole(residue * width, width), :]
    total[whole(half * rows, rows), :] += jnp.dot(data, weight, preferred_element_type=F32)


def near_kernel(own_ref, one_ref, two_refs, three_ref, four_refs, weight_ref, total):
    core, n = lax.axis_index("core"), lax.axis_size("dp")
    total[...] = jnp.zeros_like(total)
    for half in (0, 1):
        add_product(total, own_ref, half * n, half, weight_ref, lax.axis_index("zi"))
        add_product(total, one_ref, half * n, half, weight_ref, residue_at(1, core))
        add_product(total, two_refs[half], 0, half, weight_ref, residue_at(2, core))
        add_product(total, three_ref, half * n, half, weight_ref, residue_at(3, core))
        add_product(total, four_refs[half], 0, half, weight_ref, residue_at(4, core))


def up_kernel(total_in_ref, early_ref, late_ref, weight_ref, out_ref, rest_ref, total):
    core, n = lax.axis_index("core"), lax.axis_size("dp")
    total[...] = total_in_ref[...]
    for k in range(8):
        ref, at = (early_ref, late_ref)[k // 4], k % 4 * n
        add_product(total, ref, at, k % 2, weight_ref, residue_at(k // 2 + 1, 1 - core))
    columns = total.shape[1]
    row = lax.broadcasted_iota(jnp.int32, (columns, columns), 0)
    col = lax.broadcasted_iota(jnp.int32, (columns, columns), 1)
    half = columns // 2
    pick = (row == jnp.where(col < half, 2 * col, 2 * (col - half) + 1)).astype(BF16)
    out_ref[...] = jnp.dot(total[...].astype(BF16), pick, preferred_element_type=F32).astype(BF16)
    rows = rest_ref.shape[0]
    stay = total[whole(lax.axis_index("dp") * rows, rows), :]
    rest = (stay - stay.astype(BF16).astype(F32)).astype(BF16)
    rest_ref[...] = jnp.dot(rest, pick, preferred_element_type=F32).astype(BF16)


def hidden_kernel(parts_ref, rest_ref, out_ref):
    total = parts_ref[0].astype(F32) + rest_ref[...].astype(F32)
    for k in range(1, parts_ref.shape[0]):
        total += parts_ref[k].astype(F32)
    half = total.shape[1] // 2
    gate, up = total[:, :half], total[:, half:]
    out_ref[...] = (gate / (1.0 + jnp.exp(-gate)) * up).astype(BF16)


def down_kernel(hidden_ref, weight_ref, other_weight_ref, four_ref, three_ref, one_ref, two_ref, own_ref):
    core = lax.axis_index("core")
    mine, theirs = hidden_ref.at[core], hidden_ref.at[1 - core]

    def term(start, width):
        cols = pl.ds(pl.multiple_of(start, 128), width)
        out = jnp.dot(mine[...], weight_ref[:, cols], preferred_element_type=F32)
        return out + jnp.dot(theirs[...], other_weight_ref[:, cols], preferred_element_type=F32)

    width = four_ref.shape[1]
    for step, ref in zip(STEPS, (one_ref, two_ref, three_ref, four_ref)):
        ref[...] = term(residue_at(step, core) * width, width).astype(ref.dtype)
    half = own_ref.shape[1]
    own_ref[...] = term(lax.axis_index("zi") * width + core * half, half)


def give_kernel(one_ref, two_ref, out_ref):
    width = out_ref.shape[1]
    cols = whole((1 - lax.axis_index("core")) * width, width)
    out_ref[...] = one_ref[:, cols].astype(F32) + two_ref[:, cols].astype(F32)


def window_kernel(own_ref, one_ref, two_ref, given_ref, out_ref):
    core = lax.axis_index("core")
    width = own_ref.shape[1]
    cols = whole(core * width, width)
    total = own_ref[...] + one_ref[:, cols].astype(F32) + two_ref[:, cols].astype(F32)
    out_ref[...] = (total + given_ref[1 - core]).astype(BF16)


def per_device(tokens, gate_up_weight, down_weight):
    rows, width = tokens.shape
    columns = gate_up_weight.shape[1]
    dp = lax.axis_size("dp")
    shape = jax.ShapeDtypeStruct
    other_weight = swapped(down_weight)
    copies = jnp.broadcast_to(tokens[None], (dp, rows, width))
    copies = lax.all_to_all(copies, "zo", split_axis=0, concat_axis=0, tiled=True)
    copies = jnp.repeat(copies, 2, axis=0)
    pair = lax.all_to_all(copies, ("dp", "core"), split_axis=0, concat_axis=0, tiled=True)
    halves = (pair[:dp], pair[dp:])
    halves, pair = lax.optimization_barrier((halves, pair))
    first = shifted(halves[0], 2)
    second = shifted(halves[1], 2)
    one = shifted(pair, 1)
    first, other_weight = lax.optimization_barrier((first, other_weight))
    two = (first, second)
    four = tuple(shifted(a, 2, cores=(1,)) for a in two)
    three = shifted(jnp.concatenate(two), 1)
    early = swapped(jnp.concatenate([one, *two]))
    late = swapped(jnp.concatenate([three, *four]))
    total = vmem_call(
        near_kernel,
        shape((dp * rows, columns), F32),
        pair,
        one,
        two,
        three,
        four,
        gate_up_weight,
        flops=dp * rows * gate_up_weight.size,
    )
    partial_value, rest = vmem_call(
        up_kernel,
        (shape((dp * rows, columns), BF16), shape((rows, columns), BF16)),
        total,
        early,
        late,
        gate_up_weight,
        flops=dp * rows * gate_up_weight.size,
        scratch=[pltpu.VMEM((dp * rows, columns), F32)],
    )
    parts = partial_value.reshape(dp, rows, columns)
    parts = lax.all_to_all(parts, "dp", split_axis=0, concat_axis=0, tiled=True)
    own_hidden = vmem_call(
        hidden_kernel, shape((rows, columns // 2), BF16), parts, rest, flops=10 * parts.size
    )
    hidden = jnp.broadcast_to(own_hidden[None], (dp, *own_hidden.shape))
    hidden = lax.all_to_all(hidden, "dp", split_axis=0, concat_axis=0, tiled=True)
    hidden = lax.all_gather(hidden.reshape(dp * rows, columns // 2), "core", axis=0)

    block = (dp * rows, 2 * width)
    four, three, one, two, own = vmem_call(
        down_kernel,
        (shape(block, BF16),) * 3 + (shape(block, F32), shape((dp * rows, width), F32)),
        hidden,
        down_weight,
        other_weight,
        flops=4 * dp * rows * down_weight.size,
    )
    four = shifted(four, -2, cores=(1,))
    three = shifted(three, -1)
    one = shifted(one, -1)
    two = shifted((two + three.astype(F32) + four.astype(F32)).astype(BF16), -2)
    given = vmem_call(give_kernel, shape((dp * rows, width), F32), one, two, flops=2 * own.size)
    given = lax.all_gather(given, "core", axis=0)
    out = vmem_call(window_kernel, shape((dp * rows, width), BF16), own, one, two, given, flops=4 * own.size)
    out = out.reshape(dp, rows, width)
    out = lax.all_to_all(out, "dp", split_axis=0, concat_axis=0, tiled=True)
    out = lax.all_to_all(out, "zo", split_axis=0, concat_axis=0, tiled=True)
    return out.astype(F32).sum(axis=0).astype(BF16)


def solution(mesh):
    dp, tensor = mesh.shape["dp"], mesh.shape["tensor"]
    split = Mesh(
        mesh.devices.reshape(mesh.shape["groups"], dp, dp, tensor // (2 * dp), 2),
        ("groups", "dp", *TENSOR),
    )
    placed = (P(("groups", "dp"), TENSOR), P("dp", TENSOR), P(TENSOR, "dp"))
    return jax.shard_map(
        per_device,
        mesh=split,
        in_specs=placed,
        out_specs=P(("groups", "dp"), TENSOR),
        check_vma=False,
    )
```
